32 devices in a mesh: seq: 4 (over z), uly: 4 (over y, x), rep: 2 (over core).
Axes of the slice: x: 2, y: 2, z: 4, core: 2. Of those that a mesh axis runs over, the one named last changes fastest.
Arguments:
- queries: bfloat16 [4096, 2048], P(('rep', 'seq', 'uly')), parts along dimension 0, may hold values from -6 to 6
- keys: bfloat16 [4096, 2048], P(('rep', 'seq', 'uly')), parts along dimension 0, may hold values from -6 to 6
- values: bfloat16 [4096, 2048], P(('rep', 'seq', 'uly')), parts along dimension 0, may hold values from -6 to 6
- past_outputs: bfloat16 [2, 4096, 2048], P(None, ('rep', 'seq', 'uly')), parts along dimension 1, may hold values from -6 to 6
- dwa_slot: int32 [2], replicated, may hold values from 0 to 63
- dwa_table: float32 [2, 64], replicated, may hold values from 0.1 to 0.6
Outputs:
- mixed: bfloat16 [4096, 2048], P(('rep', 'seq', 'uly')), parts along dimension 0
The draws below stay inside these ranges and needn't reach their ends.
There are 2 independent parts, one for each index of `rep`. The reference program is written for one: setup_inputs(seed, part) draws one part's arguments, and reference() takes and returns one part's arrays. A program takes and returns all parts, laid end to end along the dimension named above; an argument that names none is the same for every part. Nothing has to cross between parts.
All inputs are finite; a program needn't handle non-finite values.
Results may differ from the reference program's by a relative error of at most 0.0034.
Values may be sent and summed in bfloat16 or wider, within the bound.
No kernel may reach another device: no remote copies, remote signals or barrier semaphores. Data moves between devices by JAX's collectives and lax.ppermute only.
A program may use at most 64 MiB of HBM per device.

```python
import jax
import jax.numpy as jnp
from jax import lax

HEADS = 16
HEAD_DIM = 128
PAST = 2
TABLE = 64
TOK_DEV = 128
SPAN = 4
TOKENS = 2048
N_SEQ = 4
N_ULY = 4


def drawn_pair(key):
    base = jax.random.fold_in(key, 7)
    width = HEADS * HEAD_DIM
    query_field = jnp.clip(2.5 * jax.random.normal(jax.random.fold_in(base, 1), (TOKENS, width), jnp.float32), -6.0, 6.0)
    key_field = jnp.clip(jax.random.normal(jax.random.fold_in(base, 2), (TOKENS, width), jnp.float32), -6.0, 6.0)
    return (query_field, key_field)


def draw_queries(key, part):
    return drawn_pair(key)[0].astype(jnp.bfloat16)


def draw_keys(key, part):
    return drawn_pair(key)[1].astype(jnp.bfloat16)


def block_levels(rng, shape, split, low, largest):
    factor_of, own = 1.0, jax.random.fold_in(rng, 6)
    for dim, shards_of in split:
        heights = jnp.exp(jax.random.uniform(jax.random.fold_in(own, dim), (shards_of,), jnp.float32, low / len(split), largest / len(split)))
        factor_of = factor_of * jnp.repeat(heights, shape[dim] // shards_of).reshape([-1 if axis == dim else 1 for axis in range(len(shape))])
    return factor_of


def scatter_about(stream_key, dims, spread, most, cuts=(), held_as=jnp.bfloat16):
    array = jax.random.normal(stream_key, dims, jnp.float32) * spread
    if len(cuts) > 0:
        array = block_levels(stream_key, dims, cuts, -0.22, 0.18) * array
    return jnp.clip(array, min=-most, max=most).astype(held_as)


def setup_inputs(seed: int = 0, part: int = 0) -> dict:
    key_list = jax.random.split(jax.random.key(seed), 7)
    part_keys = jax.random.split(jax.random.fold_in(key_list[6], part), 7)
    return {
        "queries": draw_queries(jax.random.fold_in(jax.random.fold_in(key_list[6], part), 71), part),
        "keys": draw_keys(jax.random.fold_in(jax.random.fold_in(key_list[6], part), 71), part),
        "values": scatter_about(part_keys[2], (TOKENS, HEADS * HEAD_DIM), 1.0, 6.0, ((0, 16),)),
        "past_outputs": scatter_about(part_keys[3], (PAST, TOKENS, HEADS * HEAD_DIM), 1.0, 6.0, ((1, 16),)),
        "dwa_slot": jax.random.randint(key_list[4], (PAST,), 0, TABLE).astype(jnp.int32),
        "dwa_table": jnp.clip(jax.random.uniform(key_list[5], (2, TABLE), jnp.float32, 0.1, 0.6), 0.1, 0.6),
    }


def one_head(items):
    query, key_block, value_block, allowed = items
    scores = jnp.dot(query, key_block.T, preferred_element_type=jnp.float32) * (1.0 / (HEAD_DIM ** 0.5))
    scores = jnp.where(allowed, scores, -jnp.inf)
    top_score = jnp.max(scores, axis=1, keepdims=True)
    prob = jnp.exp(scores - top_score)
    total = jnp.sum(prob, axis=1, keepdims=True)
    weights = prob.astype(jnp.bfloat16)
    summed = jnp.dot(weights, value_block, preferred_element_type=jnp.float32)
    return (summed / total).astype(jnp.bfloat16)


def reference(queries, keys, values, past_outputs, dwa_slot, dwa_table):
    block_rows = N_ULY * TOK_DEV

    def arrange(field):
        return field.reshape(N_SEQ, block_rows, HEADS, HEAD_DIM)

    padding = jnp.zeros((SPAN - 1, block_rows, HEADS, HEAD_DIM), jnp.bfloat16)
    query_all = arrange(queries)
    key_padded = jnp.concatenate([padding, arrange(keys)], axis=0)
    value_padded = jnp.concatenate([padding, arrange(values)], axis=0)

    def one_block(block):
        query_block = lax.dynamic_index_in_dim(query_all, block, 0, keepdims=False)
        key_window = lax.dynamic_slice_in_dim(key_padded, block, SPAN, 0).reshape(SPAN * block_rows, HEADS, HEAD_DIM)
        value_window = lax.dynamic_slice_in_dim(value_padded, block, SPAN, 0).reshape(SPAN * block_rows, HEADS, HEAD_DIM)
        query_pos = block * block_rows + jnp.arange(block_rows, dtype=jnp.int32)
        key_pos = (block - SPAN + 1) * block_rows + jnp.arange(SPAN * block_rows, dtype=jnp.int32)
        allowed = (key_pos[None, :] <= query_pos[:, None]) & (key_pos[None, :] >= 0)
        allowed_heads = jnp.broadcast_to(allowed[None, :, :], (HEADS, block_rows, SPAN * block_rows))
        result = lax.map(one_head, (jnp.transpose(query_block, (1, 0, 2)), jnp.transpose(key_window, (1, 0, 2)), jnp.transpose(value_window, (1, 0, 2)), allowed_heads))
        return jnp.transpose(result, (1, 0, 2))

    attended = lax.map(one_block, jnp.arange(N_SEQ, dtype=jnp.int32))
    attended = attended.reshape(TOKENS, HEADS * HEAD_DIM)
    coef_in = dwa_table[0][dwa_slot]
    coef_out = dwa_table[1][dwa_slot]
    layer_in = jnp.zeros((TOKENS, HEADS * HEAD_DIM), jnp.float32)
    extra = jnp.zeros((TOKENS, HEADS * HEAD_DIM), jnp.float32)
    for index in range(PAST):
        stored = past_outputs[index].astype(jnp.float32)
        layer_in = layer_in + coef_in[index] * stored
        extra = extra + coef_out[index] * stored
    hidden = layer_in + attended.astype(jnp.float32)
    return (hidden + extra).astype(jnp.bfloat16)
```

```python
import functools

import jax
import jax.numpy as jnp
from jax import lax
from jax.experimental import pallas as pl
from jax.experimental.pallas import tpu as pltpu
from jax.sharding import PartitionSpec as P

HEAD_DIM = 128
SPAN = 4
CHUNKS = 2
STAT_ROWS = 16
SCALE = 1.4426950408889634 / HEAD_DIM**0.5


def from_behind(block, axis, distance):
    devices = range(lax.axis_size(axis))
    route = [(i - distance, i) for i in devices if i - distance in devices]
    return lax.ppermute(block, axis, route)


def block_update(state, query_heads, key_heads, value_heads, allowed):
    running, total, accumulated = state
    scores = jnp.einsum("qhd,khd->hqk", query_heads, key_heads, preferred_element_type=jnp.float32)
    scores = scores * (1.0 / HEAD_DIM**0.5)
    scores = jnp.where(allowed, scores, -jnp.inf)
    new_max = jnp.maximum(running, jnp.max(scores, axis=2))
    factor = jnp.exp(running - new_max)
    prob = jnp.exp(scores - new_max[:, :, None])
    total = total * factor + jnp.sum(prob, axis=2)
    weights = prob.astype(jnp.bfloat16)
    update = jnp.einsum("hqk,khd->qhd", weights, value_heads, preferred_element_type=jnp.float32)
    accumulated = accumulated * jnp.transpose(factor)[:, :, None] + update
    return (new_max, total, accumulated)


def ring_shards(queries, keys, values, past_outputs, dwa_slot, dwa_table):
    n_uly = lax.axis_size("uly")
    n_seq = lax.axis_size("seq")
    span_size = min(SPAN, n_seq)
    features = queries.shape[1]
    local_heads = features // n_uly // HEAD_DIM
    query_rows, key_rows, value_rows = (
        lax.all_to_all(queries, "uly", split_axis=1, concat_axis=0, tiled=True),
        lax.all_to_all(keys, "uly", split_axis=1, concat_axis=0, tiled=True),
        lax.all_to_all(values, "uly", split_axis=1, concat_axis=0, tiled=True),
    )
    row_count = query_rows.shape[0]
    split_shape = (row_count, local_heads, HEAD_DIM)
    query_heads = query_rows.reshape(split_shape)
    table_index = jnp.arange(dwa_table.shape[1])
    onehot = (dwa_slot[:, None] == table_index[None, :]).astype(jnp.float32)
    coefs = jnp.dot(onehot, jnp.transpose(dwa_table), precision=lax.Precision.HIGHEST)
    layer_in = jnp.zeros(queries.shape, jnp.float32)
    extra = jnp.zeros(queries.shape, jnp.float32)
    for index in range(past_outputs.shape[0]):
        stored = past_outputs[index].astype(jnp.float32)
        layer_in = layer_in + coefs[index, 0] * stored
        extra = extra + coefs[index, 1] * stored
    running = jnp.full((local_heads, row_count), -jnp.inf, jnp.float32)
    total = jnp.zeros((local_heads, row_count), jnp.float32)
    accumulated = jnp.zeros(split_shape, jnp.float32)
    state = (running, total, accumulated)
    causal = (jnp.arange(row_count)[:, None] >= jnp.arange(row_count)[None, :])[None, :, :]
    state = block_update(
        state, query_heads, key_rows.reshape(split_shape), value_rows.reshape(split_shape), causal
    )
    position = lax.axis_index("seq")
    current = (key_rows, value_rows)
    for offset in range(1, span_size):
        current = from_behind((current[0], current[1]), "seq", 1)
        far_keys = current[0].reshape(split_shape)
        far_values = current[1].reshape(split_shape)

        def take_block(carry, far_keys=far_keys, far_values=far_values):
            return block_update(carry, query_heads, far_keys, far_values, True)

        def keep_block(carry):
            return carry

        state = lax.cond(position >= offset, take_block, keep_block, state)
    running, total, accumulated = state
    attended = accumulated / jnp.transpose(total)[:, :, None]
    attended = attended.astype(jnp.bfloat16).reshape(row_count, local_heads * HEAD_DIM)
    returned = lax.all_to_all(attended, "uly", split_axis=0, concat_axis=1, tiled=True)
    hidden = layer_in + returned.astype(jnp.float32)
    return (hidden + extra).astype(jnp.bfloat16)


def pack_kernel(where, q, k, v, *outs):
    width = outs[0].shape[2]
    n = len(outs) // CHUNKS
    for s in range(n):
        for c in range(CHUNKS):
            start = pl.multiple_of((where[1] ^ s) * (width * CHUNKS) + c * width, HEAD_DIM)
            for t, ref in enumerate((q, k, v)):
                outs[c * n + s][t] = ref[:, pl.ds(start, width)]


def attend(query, blocks, allowed):
    scores = []
    for key, _ in blocks:
        scores.append(lax.dot_general(key, query, (((1,), (1,)), ((), ())), preferred_element_type=jnp.float32))
    if allowed is not None:
        scores[-1] = jnp.where(allowed, scores[-1], -jnp.inf)
    top = jnp.max(scores[0], axis=0, keepdims=True)
    for other in scores[1:]:
        top = jnp.maximum(top, jnp.max(other, axis=0, keepdims=True))
    total, summed = 0.0, 0.0
    for score, (_, value) in zip(scores, blocks):
        prob = jnp.exp2((score - top) * SCALE)
        total = total + jnp.sum(prob, axis=0, keepdims=True)
        summed = summed + lax.dot_general(
            value, prob.astype(jnp.bfloat16), (((0,), (0,)), ((), ())), preferred_element_type=jnp.float32
        )
    return summed / total, top * SCALE + jnp.log2(total)


def attention_kernel(part, where, q, kv, far, qa, qb, own, lse, ra, rb):
    z, u = where[0], where[1]
    rows = q.shape[0]
    spot = lambda axis: lax.broadcasted_iota(jnp.int32, (rows, rows), axis)
    place = lambda i: (((i // part) ^ u) * part) + i % part
    near = (kv[0], kv[1])
    odd = z % 2 == 1

    def put(result):
        own[0] = result[0]
        lse[0] = jnp.broadcast_to(result[1], lse.shape[1:])

    def send(out, result):
        out[0, :HEAD_DIM] = result[0].astype(jnp.bfloat16)
        high = result[1].astype(jnp.bfloat16).astype(jnp.float32)
        middle = (result[1] - high).astype(jnp.bfloat16).astype(jnp.float32)
        low = result[1] - high - middle
        row = lax.broadcasted_iota(jnp.int32, (STAT_ROWS, rows), 0)
        stats = jnp.where(row == 0, high, jnp.where(row == 1, middle, jnp.where(row == 2, low, 0.0)))
        out[0, HEAD_DIM:] = stats.astype(jnp.bfloat16)

    @pl.when(z == 1)
    def _():
        send(rb, attend(qb[...], [(far[0], far[1]), near], None))
        send(ra, attend(qa[...], [(far[0], far[1]), near], None))

    @pl.when(odd)
    def _():
        allowed = place(spot(1)) >= place(spot(0))
        put(attend(q[...], [(far[0], far[1]), near], allowed))

    @pl.when(jnp.logical_not(odd))
    def _():
        allowed = place(spot(1)) >= place(spot(0))
        put(attend(q[...], [near], allowed))


def merge_kernel(where, own, lse, ra, rb, *outs):
    z = where[0]

    def write(result):
        tokens = jnp.transpose(result).astype(jnp.bfloat16)
        rows = outs[0].shape[0]
        for s, out in enumerate(outs):
            out[...] = tokens[s * rows : (s + 1) * rows]

    def merged(ref):
        stats = ref[0, HEAD_DIM:].astype(jnp.float32)
        other = stats[0:1] + stats[1:2] + stats[2:3]
        mine = lse[0, 0:1]
        top = jnp.maximum(mine, other)
        w_mine, w_other = jnp.exp2(mine - top), jnp.exp2(other - top)
        scale = 1.0 / (w_mine + w_other)
        write(own[0] * (w_mine * scale) + ref[0, :HEAD_DIM].astype(jnp.float32) * (w_other * scale))

    pl.when(z < 2)(lambda: write(own[0]))
    pl.when(z == 2)(lambda: merged(ra))
    pl.when(z == 3)(lambda: merged(rb))


def mix_kernel(where, slot, table, past, *refs):
    out, parts = refs[-1], refs[:-1]
    n = len(parts) // CHUNKS
    width = parts[0].shape[1]
    coefs = [table[0, slot[p]] + table[1, slot[p]] for p in range(past.shape[0])]
    for s in range(n):
        for c in range(CHUNKS):
            cols = pl.ds(pl.multiple_of((where[1] ^ s) * (width * CHUNKS) + c * width, HEAD_DIM), width)
            acc = parts[c * n + s][...].astype(jnp.float32)
            for p, coef in enumerate(coefs):
                acc = acc + coef * past[p, :, cols].astype(jnp.float32)
            out[:, cols] = acc.astype(jnp.bfloat16)


SMEM = pl.BlockSpec(memory_space=pltpu.SMEM)
VMEM = pl.BlockSpec(memory_space=pltpu.VMEM)


def shards(queries, keys, values, past_outputs, dwa_slot, dwa_table):
    n_uly, n_seq = lax.axis_size("uly"), lax.axis_size("seq")
    rows, features = queries.shape
    heads = features // n_uly // HEAD_DIM
    if n_seq != 4 or n_uly & (n_uly - 1) or heads % CHUNKS:
        return ring_shards(queries, keys, values, past_outputs, dwa_slot, dwa_table)
    where = jnp.stack([lax.axis_index("seq"), lax.axis_index("uly")]).astype(jnp.int32)
    hc = heads // CHUNKS
    width = hc * HEAD_DIM
    block = n_uly * rows
    bf16, f32 = jnp.bfloat16, jnp.float32
    shape = jax.ShapeDtypeStruct

    def swap(array, s):
        return lax.ppermute(array, "uly", [(i, i ^ s) for i in range(n_uly)])

    packed = pl.pallas_call(
        pack_kernel,
        in_specs=[SMEM, VMEM, VMEM, VMEM],
        out_specs=[VMEM] * (CHUNKS * n_uly),
        out_shape=[shape((3, rows, width), bf16)] * (CHUNKS * n_uly),
    )(where, queries, keys, values)

    def head_block(count):
        return pl.BlockSpec((count, block, HEAD_DIM), lambda h: (0, 0, h))

    flat = pl.BlockSpec((block, HEAD_DIM), lambda h: (0, h))

    def per_head(size):
        return pl.BlockSpec((1, size, block), lambda h: (h, 0, 0))

    arrived = [[packed[c * n_uly + s] if s == 0 else swap(packed[c * n_uly + s], s) for s in range(n_uly)] for c in range(CHUNKS)]
    results = []
    for c in range(CHUNKS):
        q = jnp.concatenate([a[0] for a in arrived[c]], axis=0)
        kv = jnp.concatenate([a[1:3] for a in arrived[c]], axis=1)
        qb = lax.ppermute(q, "seq", [(3, 1)])
        qa = lax.ppermute(q, "seq", [(2, 1)])
        far = lax.ppermute(kv, "seq", [(0, 1), (2, 3)])
        own, lse, ra, rb = pl.pallas_call(
            functools.partial(attention_kernel, rows),
            grid=(hc,),
            in_specs=[SMEM, flat, head_block(2), head_block(2), flat, flat],
            out_specs=[per_head(HEAD_DIM), per_head(8), per_head(HEAD_DIM + STAT_ROWS), per_head(HEAD_DIM + STAT_ROWS)],
            out_shape=[
                shape((hc, HEAD_DIM, block), f32),
                shape((hc, 8, block), f32),
                shape((hc, HEAD_DIM + STAT_ROWS, block), bf16),
                shape((hc, HEAD_DIM + STAT_ROWS, block), bf16),
            ],
        )(where, q, kv, far, qa, qb)
        rb = lax.ppermute(rb, "seq", [(1, 3)])
        ra = lax.ppermute(ra, "seq", [(1, 2)])
        outs = pl.pallas_call(
            merge_kernel,
            grid=(hc,),
            in_specs=[SMEM, per_head(HEAD_DIM), per_head(8), per_head(HEAD_DIM + STAT_ROWS), per_head(HEAD_DIM + STAT_ROWS)],
            out_specs=[pl.BlockSpec((rows, HEAD_DIM), lambda h: (0, h))] * n_uly,
            out_shape=[shape((rows, width), bf16)] * n_uly,
        )(where, own, lse, ra, rb)
        results += [out if s == 0 else swap(out, s) for s, out in enumerate(outs)]
    return pl.pallas_call(
        mix_kernel,
        in_specs=[SMEM, SMEM, SMEM] + [VMEM] * (1 + len(results)),
        out_specs=VMEM,
        out_shape=shape((rows, features), bf16),
    )(where, dwa_slot, dwa_table, past_outputs, *results)


def solution(mesh):
    return jax.shard_map(
        shards,
        mesh=mesh,
        in_specs=(
            P(("rep", "seq", "uly"), None),
            P(("rep", "seq", "uly"), None),
            P(("rep", "seq", "uly"), None),
            P(None, ("rep", "seq", "uly"), None),
            P(),
            P(),
        ),
        out_specs=P(("rep", "seq", "uly"), None),
        check_vma=False,
    )
```

```python
import functools

import jax
import jax.numpy as jnp
from jax import lax
from jax.experimental import pallas as pl
from jax.experimental.pallas import tpu as pltpu
from jax.sharding import PartitionSpec as P

HEAD_DIM = 128
SPAN = 4
CHUNKS = 2
STAT_ROWS = 16
SCALE = 1.4426950408889634 / HEAD_DIM**0.5


def from_behind(block, axis, distance):
    devices = range(lax.axis_size(axis))
    route = [(i - distance, i) for i in devices if i - distance in devices]
    return lax.ppermute(block, axis, route)


def block_update(state, query_heads, key_heads, value_heads, allowed):
    running, total, accumulated = state
    scores = jnp.einsum("qhd,khd->hqk", query_heads, key_heads, preferred_element_type=jnp.float32)
    scores = scores * (1.0 / HEAD_DIM**0.5)
    scores = jnp.where(allowed, scores, -jnp.inf)
    new_max = jnp.maximum(running, jnp.max(scores, axis=2))
    factor = jnp.exp(running - new_max)
    prob = jnp.exp(scores - new_max[:, :, None])
    total = total * factor + jnp.sum(prob, axis=2)
    weights = prob.astype(jnp.bfloat16)
    update = jnp.einsum("hqk,khd->qhd", weights, value_heads, preferred_element_type=jnp.float32)
    accumulated = accumulated * jnp.transpose(factor)[:, :, None] + update
    return (new_max, total, accumulated)


def ring_shards(queries, keys, values, past_outputs, dwa_slot, dwa_table):
    n_uly = lax.axis_size("uly")
    n_seq = lax.axis_size("seq")
    span_size = min(SPAN, n_seq)
    features = queries.shape[1]
    local_heads = features // n_uly // HEAD_DIM
    query_rows, key_rows, value_rows = (
        lax.all_to_all(queries, "uly", split_axis=1, concat_axis=0, tiled=True),
        lax.all_to_all(keys, "uly", split_axis=1, concat_axis=0, tiled=True),
        lax.all_to_all(values, "uly", split_axis=1, concat_axis=0, tiled=True),
    )
    row_count = query_rows.shape[0]
    split_shape = (row_count, local_heads, HEAD_DIM)
    query_heads = query_rows.reshape(split_shape)
    table_index = jnp.arange(dwa_table.shape[1])
    onehot = (dwa_slot[:, None] == table_index[None, :]).astype(jnp.float32)
    coefs = jnp.dot(onehot, jnp.transpose(dwa_table), precision=lax.Precision.HIGHEST)
    layer_in = jnp.zeros(queries.shape, jnp.float32)
    extra = jnp.zeros(queries.shape, jnp.float32)
    for index in range(past_outputs.shape[0]):
        stored = past_outputs[index].astype(jnp.float32)
        layer_in = layer_in + coefs[index, 0] * stored
        extra = extra + coefs[index, 1] * stored
    running = jnp.full((local_heads, row_count), -jnp.inf, jnp.float32)
    total = jnp.zeros((local_heads, row_count), jnp.float32)
    accumulated = jnp.zeros(split_shape, jnp.float32)
    state = (running, total, accumulated)
    causal = (jnp.arange(row_count)[:, None] >= jnp.arange(row_count)[None, :])[None, :, :]
    state = block_update(
        state, query_heads, key_rows.reshape(split_shape), value_rows.reshape(split_shape), causal
    )
    position = lax.axis_index("seq")
    current = (key_rows, value_rows)
    for offset in range(1, span_size):
        current = from_behind((current[0], current[1]), "seq", 1)
        far_keys = current[0].reshape(split_shape)
        far_values = current[1].reshape(split_shape)

        def take_block(carry, far_keys=far_keys, far_values=far_values):
            return block_update(carry, query_heads, far_keys, far_values, True)

        def keep_block(carry):
            return carry

        state = lax.cond(position >= offset, take_block, keep_block, state)
    running, total, accumulated = state
    attended = accumulated / jnp.transpose(total)[:, :, None]
    attended = attended.astype(jnp.bfloat16).reshape(row_count, local_heads * HEAD_DIM)
    returned = lax.all_to_all(attended, "uly", split_axis=0, concat_axis=1, tiled=True)
    hidden = layer_in + returned.astype(jnp.float32)
    return (hidden + extra).astype(jnp.bfloat16)


def pack_kernel(q, k, v, *outs):
    width = outs[0].shape[2]
    n = len(outs) // CHUNKS
    for s in range(n):
        for c in range(CHUNKS):
            start = pl.multiple_of((lax.axis_index("uly") ^ s) * (width * CHUNKS) + c * width, HEAD_DIM)
            for t, ref in enumerate((q, k, v)):
                outs[c * n + s][t] = ref[:, pl.ds(start, width)]


def attend(query, blocks, allowed):
    scores = []
    for key, _ in blocks:
        scores.append(lax.dot_general(key, query, (((1,), (1,)), ((), ())), preferred_element_type=jnp.float32))
    if allowed is not None:
        scores[-1] = jnp.where(allowed, scores[-1], -jnp.inf)
    top = jnp.max(scores[0], axis=0, keepdims=True)
    for other in scores[1:]:
        top = jnp.maximum(top, jnp.max(other, axis=0, keepdims=True))
    total, summed = 0.0, 0.0
    for score, (_, value) in zip(scores, blocks):
        prob = jnp.exp2((score - top) * SCALE)
        total = total + jnp.sum(prob, axis=0, keepdims=True)
        summed = summed + lax.dot_general(
            value, prob.astype(jnp.bfloat16), (((0,), (0,)), ((), ())), preferred_element_type=jnp.float32
        )
    return summed / total, top * SCALE + jnp.log2(total)


def attention_kernel(part, q, kv, far, qa, qb, own, lse, ra, rb):
    z, u = lax.axis_index("seq"), lax.axis_index("uly")
    rows = q.shape[0]
    spot = lambda axis: lax.broadcasted_iota(jnp.int32, (rows, rows), axis)
    place = lambda i: (((i // part) ^ u) * part) + i % part
    near = (kv[0], kv[1])
    odd = z % 2 == 1

    def put(result):
        own[0] = result[0]
        lse[0] = jnp.broadcast_to(result[1], lse.shape[1:])

    def send(out, result):
        out[0, :HEAD_DIM] = result[0].astype(jnp.bfloat16)
        high = result[1].astype(jnp.bfloat16).astype(jnp.float32)
        middle = (result[1] - high).astype(jnp.bfloat16).astype(jnp.float32)
        low = result[1] - high - middle
        row = lax.broadcasted_iota(jnp.int32, (STAT_ROWS, rows), 0)
        stats = jnp.where(row == 0, high, jnp.where(row == 1, middle, jnp.where(row == 2, low, 0.0)))
        out[0, HEAD_DIM:] = stats.astype(jnp.bfloat16)

    @pl.when(z == 1)
    def _():
        send(rb, attend(qb[...], [(far[0], far[1]), near], None))
        send(ra, attend(qa[...], [(far[0], far[1]), near], None))

    @pl.when(odd)
    def _():
        allowed = place(spot(1)) >= place(spot(0))
        put(attend(q[...], [(far[0], far[1]), near], allowed))

    @pl.when(jnp.logical_not(odd))
    def _():
        allowed = place(spot(1)) >= place(spot(0))
        put(attend(q[...], [near], allowed))


def merge_kernel(own, lse, ra, rb, *outs):
    z = lax.axis_index("seq")

    def write(result):
        tokens = jnp.transpose(result).astype(jnp.bfloat16)
        rows = outs[0].shape[0]
        for s, out in enumerate(outs):
            out[...] = tokens[s * rows : (s + 1) * rows]

    def merged(ref):
        stats = ref[0, HEAD_DIM:].astype(jnp.float32)
        other = stats[0:1] + stats[1:2] + stats[2:3]
        mine = lse[0, 0:1]
        top = jnp.maximum(mine, other)
        w_mine, w_other = jnp.exp2(mine - top), jnp.exp2(other - top)
        scale = 1.0 / (w_mine + w_other)
        write(own[0] * (w_mine * scale) + ref[0, :HEAD_DIM].astype(jnp.float32) * (w_other * scale))

    pl.when(z < 2)(lambda: write(own[0]))
    pl.when(z == 2)(lambda: merged(ra))
    pl.when(z == 3)(lambda: merged(rb))


def mix_kernel(slot, table, past, *refs):
    out, parts = refs[-1], refs[:-1]
    n = len(parts) // CHUNKS
    width = parts[0].shape[1]
    coefs = [table[0, slot[p]] + table[1, slot[p]] for p in range(past.shape[0])]
    for s in range(n):
        for c in range(CHUNKS):
            cols = pl.ds(pl.multiple_of((lax.axis_index("uly") ^ s) * (width * CHUNKS) + c * width, HEAD_DIM), width)
            acc = parts[c * n + s][...].astype(jnp.float32)
            for p, coef in enumerate(coefs):
                acc = acc + coef * past[p, :, cols].astype(jnp.float32)
            out[:, cols] = acc.astype(jnp.bfloat16)


SMEM = pl.BlockSpec(memory_space=pltpu.SMEM)
VMEM = pl.BlockSpec(memory_space=pltpu.VMEM)


def shards(queries, keys, values, past_outputs, dwa_slot, dwa_table):
    n_uly, n_seq = lax.axis_size("uly"), lax.axis_size("seq")
    rows, features = queries.shape
    heads = features // n_uly // HEAD_DIM
    if n_seq != 4 or n_uly & (n_uly - 1) or heads % CHUNKS:
        return ring_shards(queries, keys, values, past_outputs, dwa_slot, dwa_table)
    hc = heads // CHUNKS
    width = hc * HEAD_DIM
    block = n_uly * rows
    bf16, f32 = jnp.bfloat16, jnp.float32
    shape = jax.ShapeDtypeStruct

    def swap(array, s):
        return lax.ppermute(array, "uly", [(i, i ^ s) for i in range(n_uly)])

    packed = pl.pallas_call(
        pack_kernel,
        in_specs=[VMEM] * 3,
        out_specs=[VMEM] * (CHUNKS * n_uly),
        out_shape=[shape((3, rows, width), bf16)] * (CHUNKS * n_uly),
    )(queries, keys, values)

    def head_block(count):
        return pl.BlockSpec((count, block, HEAD_DIM), lambda h: (0, 0, h))

    flat = pl.BlockSpec((block, HEAD_DIM), lambda h: (0, h))

    def per_head(size):
        return pl.BlockSpec((1, size, block), lambda h: (h, 0, 0))

    arrived = [[packed[c * n_uly + s] if s == 0 else swap(packed[c * n_uly + s], s) for s in range(n_uly)] for c in range(CHUNKS)]
    results = []
    for c in range(CHUNKS):
        q = jnp.concatenate([a[0] for a in arrived[c]], axis=0)
        kv = jnp.concatenate([a[1:3] for a in arrived[c]], axis=1)
        qb = lax.ppermute(q, "seq", [(3, 1)])
        qa = lax.ppermute(q, "seq", [(2, 1)])
        far = lax.ppermute(kv, "seq", [(0, 1), (2, 3)])
        own, lse, ra, rb = pl.pallas_call(
            functools.partial(attention_kernel, rows),
            grid=(hc,),
            in_specs=[flat, head_block(2), head_block(2), flat, flat],
            out_specs=[per_head(HEAD_DIM), per_head(8), per_head(HEAD_DIM + STAT_ROWS), per_head(HEAD_DIM + STAT_ROWS)],
            out_shape=[
                shape((hc, HEAD_DIM, block), f32),
                shape((hc, 8, block), f32),
                shape((hc, HEAD_DIM + STAT_ROWS, block), bf16),
                shape((hc, HEAD_DIM + STAT_ROWS, block), bf16),
            ],
        )(q, kv, far, qa, qb)
        rb = lax.ppermute(rb, "seq", [(1, 3)])
        ra = lax.ppermute(ra, "seq", [(1, 2)])
        outs = pl.pallas_call(
            merge_kernel,
            grid=(hc,),
            in_specs=[per_head(HEAD_DIM), per_head(8), per_head(HEAD_DIM + STAT_ROWS), per_head(HEAD_DIM + STAT_ROWS)],
            out_specs=[pl.BlockSpec((rows, HEAD_DIM), lambda h: (0, h))] * n_uly,
            out_shape=[shape((rows, width), bf16)] * n_uly,
        )(own, lse, ra, rb)
        results += [out if s == 0 else swap(out, s) for s, out in enumerate(outs)]
    return pl.pallas_call(
        mix_kernel,
        in_specs=[SMEM, SMEM] + [VMEM] * (1 + len(results)),
        out_specs=VMEM,
        out_shape=shape((rows, features), bf16),
    )(dwa_slot, dwa_table, past_outputs, *results)


def solution(mesh):
    return jax.shard_map(
        shards,
        mesh=mesh,
        in_specs=(
            P(("rep", "seq", "uly"), None),
            P(("rep", "seq", "uly"), None),
            P(("rep", "seq", "uly"), None),
            P(None, ("rep", "seq", "uly"), None),
            P(),
            P(),
        ),
        out_specs=P(("rep", "seq", "uly"), None),
        check_vma=False,
    )
```
